32 devices in a mesh: prow: 4 (over x, core), pcol: 8 (over z, y).
Axes of the slice: x: 2, y: 2, z: 4, core: 2. Of those that a mesh axis runs over, the one named last changes fastest.
Arguments:
- slab: float32 [16384, 2048], P('prow', 'pcol'), may hold values from -6 to 6
- panel: float32 [16384, 512], P(('prow', 'pcol')), may hold values from -0.25 to 0.25
- pivots: int32 [512], replicated, may hold values from 0 to 16383, as said below
- inv_lower: float32 [512, 512], replicated, as said below
- inv_upper: float32 [512, 512], replicated, as said below
Outputs:
- updated: float32 [16384, 2048], P('prow', 'pcol')
The draws below stay inside these ranges and needn't reach their ends.
Inputs may be any that keep to these rules, and one draw needn't show every extreme that they name: `pivots`: 512 distinct row indices. `inv_lower`: unit lower triangular. `inv_upper`: upper triangular with a positive diagonal.
All inputs are finite; a program needn't handle non-finite values.
Results may differ from the reference program's by a relative error of at most 0.000061.
Values sent between devices are 32-bit elements; how exact they have to be, the bound alone decides.
No kernel may reach another device: no remote copies, remote signals or barrier semaphores. Data moves between devices by JAX's collectives and lax.ppermute only.
A program may use at most 64 MiB of HBM per device.

```python
import jax
import jax.numpy as jnp
from jax import lax

NB = 512
ROWS_DEV = 4096
NS_DEV = 256
M = 16384
NS = 2048
N_PROW = 4
N_PCOL = 8


def draw_pivots(key, part):
    order = jax.random.permutation(jax.random.fold_in(key, 11), ROWS_DEV * N_PROW)
    return order[:NB].astype(jnp.int32)


def draw_inv_lower(key, part):
    sub_key = jax.random.fold_in(key, 23)
    entries = jax.random.normal(sub_key, (NB, NB), jnp.float32)
    return jnp.tril(entries, -1) * NB ** (-0.5) + jnp.eye(NB, dtype=jnp.float32)


def draw_inv_upper(key, part):
    sub_key = jax.random.fold_in(key, 37)
    diag_key = jax.random.fold_in(key, 41)
    entries = jax.random.normal(sub_key, (NB, NB), jnp.float32)
    diagonal = jax.random.uniform(diag_key, (NB,), jnp.float32, 0.5, 1.5)
    return jnp.triu(entries, 1) * NB ** (-0.5) + jnp.diag(diagonal)


def shard_levels(key, extent, split, least, high):
    def one(dim, parts):
        steps = jax.random.uniform(jax.random.fold_in(jax.random.fold_in(key, 6), dim), (parts,), jnp.float32, least / len(split), high / len(split))
        return jnp.repeat(jnp.exp(steps), extent[dim] // parts).reshape((-1,) + (1,) * (len(extent) - dim - 1))

    gain = one(*split[0])
    for cut in split[1:]:
        gain = gain * one(*cut)
    return gain


def normal_values(rng, shape, scale, bound, split=(), kind=jnp.bfloat16):
    values = scale * jax.random.normal(rng, shape, jnp.float32)
    if split:
        values = values * shard_levels(rng, shape, split, -0.22, 0.18)
    return jnp.clip(values, -bound, bound).astype(kind)


def setup_inputs(seed: int = 0) -> dict:
    arg_keys = jax.random.split(jax.random.key(seed), 6)
    return {
        "slab": normal_values(arg_keys[0], (M, NS), 1.0, 6.0, ((0, 4), (1, 8)), jnp.float32),
        "panel": normal_values(arg_keys[1], (M, NB), NB ** -0.5, 0.25, ((0, 32),), jnp.float32),
        "pivots": draw_pivots(jax.random.fold_in(arg_keys[5], 71), 0),
        "inv_lower": draw_inv_lower(jax.random.fold_in(arg_keys[5], 71), 0),
        "inv_upper": draw_inv_upper(jax.random.fold_in(arg_keys[5], 71), 0),
    }


def reference(slab, panel, pivots, inv_lower, inv_upper):
    pivot_rows = jnp.take(slab, pivots.astype(jnp.int32), axis=0)
    upper_block = jnp.dot(inv_lower, pivot_rows, precision=lax.Precision.HIGHEST, preferred_element_type=jnp.float32)
    panel_blocks = panel.reshape(N_PROW, ROWS_DEV, NB)
    slab_blocks = slab.reshape(N_PROW, ROWS_DEV, NS_DEV * N_PCOL)

    def one_block(operands):
        panel_block, slab_block = operands
        lower_rows = jnp.dot(panel_block, inv_upper, precision=lax.Precision.HIGHEST, preferred_element_type=jnp.float32)
        product = jnp.dot(lower_rows, upper_block, precision=lax.Precision.HIGHEST, preferred_element_type=jnp.float32)
        return slab_block - product

    updated = lax.map(one_block, (panel_blocks, slab_blocks)).reshape(slab.shape)
    updated = updated.at[pivots.astype(jnp.int32)].set(upper_block)
    return updated
```

```python
import functools

import jax
import jax.numpy as jnp
import numpy as np
from jax import lax
from jax.experimental import pallas as pl
from jax.experimental.pallas import tpu as pltpu
from jax.sharding import PartitionSpec as P


def split(value):
    high = value.astype(jnp.bfloat16)
    low = (value - high.astype(jnp.float32)).astype(jnp.bfloat16)
    return high, low


def dot3(left, right):
    dot = functools.partial(jnp.dot, preferred_element_type=jnp.float32)
    return dot(left[0], right[0]) + (dot(left[0], right[1]) + dot(left[1], right[0]))


def prepare_kernel(lower_ref, first_ref, second_ref, upper_ref, uh_ref, ul_ref, ih_ref, il_ref):
    rows = split(first_ref[...] + second_ref[...])
    uh_ref[...], ul_ref[...] = split(dot3(split(lower_ref[...]), rows))
    ih_ref[...], il_ref[...] = split(upper_ref[...])


def prepare(inv_lower, first, second, inv_upper):
    depth, cols = first.shape
    return pl.pallas_call(
        prepare_kernel,
        out_shape=[
            jax.ShapeDtypeStruct((depth, cols), jnp.bfloat16),
            jax.ShapeDtypeStruct((depth, cols), jnp.bfloat16),
            jax.ShapeDtypeStruct((depth, depth), jnp.bfloat16),
            jax.ShapeDtypeStruct((depth, depth), jnp.bfloat16),
        ],
        cost_estimate=pl.CostEstimate(
            flops=6 * depth * depth * cols, bytes_accessed=8 * depth * (depth + cols), transcendentals=0
        ),
        name="prepare",
    )(inv_lower, first, second, inv_upper)


def update_kernel(base, table, piece_ref, ih_ref, il_ref, uh_ref, ul_ref, piv_ref, slab_ref, *refs):
    out_ref = refs[-1]
    block = piece_ref.shape[0]
    solved = dot3(split(piece_ref[...]), (ih_ref[...], il_ref[...]))
    start = table[base + pl.program_id(0)] * block
    row = start + lax.broadcasted_iota(jnp.int32, solved.shape, 0)
    hit = row == piv_ref[...]
    is_pivot = jnp.max(jnp.where(hit, 1.0, 0.0), axis=1, keepdims=True) > 0.0
    solved = jnp.where(is_pivot, jnp.where(hit, -1.0, 0.0), solved)
    product = dot3(split(solved), (uh_ref[...], ul_ref[...]))
    out_ref[...] = jnp.where(is_pivot, 0.0, slab_ref[...]) - product


def update(base, block, table, piece, factors, pivots, slab, previous):
    rows, depth = piece.shape
    cols = slab.shape[1]
    whole = lambda shape: pl.BlockSpec(shape, lambda i, table: (0, 0))
    moved = pl.BlockSpec((block, cols), lambda i, table: (table[base + i], 0))
    in_specs = [
        pl.BlockSpec((block, depth), lambda i, table: (i, 0)),
        whole((depth, depth)),
        whole((depth, depth)),
        whole((depth, cols)),
        whole((depth, cols)),
        whole((1, depth)),
        moved,
    ]
    uh, ul, ih, il = factors
    operands = [table, piece, ih, il, uh, ul, pivots, slab]
    aliases = {}
    if previous is not None:
        in_specs.append(pl.BlockSpec(memory_space=pl.ANY))
        aliases = {len(operands): 0}
        operands.append(previous)
    return pl.pallas_call(
        functools.partial(update_kernel, base),
        grid_spec=pltpu.PrefetchScalarGridSpec(
            num_scalar_prefetch=1, grid=(rows // block,), in_specs=in_specs, out_specs=moved
        ),
        out_shape=jax.ShapeDtypeStruct(slab.shape, jnp.float32),
        input_output_aliases=aliases,
        cost_estimate=pl.CostEstimate(
            flops=6 * rows * depth * (depth + cols),
            bytes_accessed=4 * (rows * (depth + 2 * cols) + depth * (depth + cols)),
            transcendentals=0,
        ),
        name="update",
    )(*operands)


def gather_plan(panel, n_pcol):
    rows = panel.shape[0]
    inner, outer = 2, n_pcol // 2
    if outer != 4 or rows % 512:
        whole = lax.all_gather(panel, "pcol", axis=0, tiled=True)
        return [(whole, [(None, j, 0) for j in range(n_pcol)], rows)]
    flip = [(z * inner + y, z * inner + 1 - y) for z in range(outer) for y in range(inner)]
    plus = [(z * inner + y, (z + 1) % outer * inner + y) for z in range(outer) for y in range(inner)]
    minus = [(b, a) for a, b in plus]
    send = lambda value, pairs: lax.ppermute(value, "pcol", pairs)
    half, most = rows // 2, rows * 3 // 4
    back = send(panel, plus)
    ahead = send(panel, minus)
    side = send(panel, flip)
    far_top = send(back[:half], plus)
    far_bottom = send(ahead[half:], minus)
    corners = send(jnp.concatenate([back[most:], ahead[most:]]), flip)
    side_most = side[:most]
    back_side = send(side_most, plus)
    ahead_side = send(side_most, minus)
    far_side_top = send(far_top, flip)
    far_side_bottom = send(far_bottom, flip)
    quarter = rows - most
    return [
        (panel, [(0, 0, 0)], rows),
        (back, [(-1, 0, 0)], rows),
        (ahead, [(1, 0, 0)], rows),
        (side, [(0, 1, 0)], rows),
        (far_top, [(2, 0, 0)], half),
        (far_bottom, [(2, 0, half)], half),
        (corners, [(-1, 1, most), (1, 1, most)], quarter),
        (far_side_top, [(2, 1, 0)], half),
        (back_side, [(-1, 1, 0)], most),
        (ahead_side, [(1, 1, 0)], most),
        (far_side_bottom, [(2, 1, half)], half),
    ]


def sum_over_prow(value, n_prow):
    if n_prow & (n_prow - 1) or n_prow < 2:
        total = lax.psum(value, "prow")
        return total, jnp.zeros_like(total)
    step = 1
    while True:
        other = lax.ppermute(value, "prow", [(i, i ^ step) for i in range(n_prow)])
        step *= 2
        if step == n_prow:
            return value, other
        value = value + other


def local(n_prow, n_pcol, slab, panel, pivots, inv_lower, inv_upper):
    row_count = slab.shape[0]
    pieces = gather_plan(panel, n_pcol)

    local_index = pivots - lax.axis_index("prow") * row_count
    inside = (local_index >= 0) & (local_index < row_count)
    safe_index = jnp.where(inside, local_index, 0)
    picked = jnp.where(inside[:, None], jnp.take(slab, safe_index, axis=0), 0.0)
    factors = prepare(inv_lower, *sum_over_prow(picked, n_prow), inv_upper)

    shifts, flips, starts, divisors, plan = [], [], [], [], []
    absolute = []
    for piece, runs, length in pieces:
        block = next(b for b in (256, 128, 64, 32, 16, 8) if length % b == 0 and all(r[2] % b == 0 for r in runs))
        plan.append((len(starts), block))
        for shift, flip, offset in runs:
            for part in range(length // block):
                absolute.append(shift is None)
                shifts.append(shift or 0)
                flips.append(flip)
                starts.append(offset + part * block)
                divisors.append(block)
    me = lax.axis_index("pcol")
    if absolute[0]:
        owner = np.array(flips, np.int32)
    else:
        owner = (me // 2 + np.array(shifts, np.int32) + n_pcol) % (n_pcol // 2) * 2 + (me % 2 ^ np.array(flips, np.int32))
    table = ((owner * panel.shape[0] + np.array(starts, np.int32)) // np.array(divisors, np.int32)).astype(jnp.int32)
    table = jnp.asarray(table)

    updated = None
    for (piece, _, _), (base, block) in zip(pieces, plan):
        updated = update(base, block, table, piece, factors, local_index[None, :], slab, updated)
    return updated


def solution(mesh):
    return jax.shard_map(
        functools.partial(local, mesh.shape["prow"], mesh.shape["pcol"]),
        mesh=mesh,
        in_specs=(P("prow", "pcol"), P(("prow", "pcol"), None), P(), P(), P()),
        out_specs=P("prow", "pcol"),
        check_vma=False,
    )
```

```python
import functools

import jax
import jax.numpy as jnp
import numpy as np
from jax import lax
from jax.experimental import pallas as pl
from jax.experimental.pallas import tpu as pltpu
from jax.sharding import PartitionSpec as P


def split(value):
    high = value.astype(jnp.bfloat16)
    low = (value - high.astype(jnp.float32)).astype(jnp.bfloat16)
    return high, low


def dot3(left, right):
    dot = functools.partial(jnp.dot, preferred_element_type=jnp.float32)
    return dot(left[0], right[0]) + (dot(left[0], right[1]) + dot(left[1], right[0]))


def cost(flops, moved):
    return pl.CostEstimate(flops=flops, bytes_accessed=moved, transcendentals=0)


def hits(first_row, rows, piv_ref):
    depth = piv_ref.shape[1]
    row = first_row + lax.broadcasted_iota(jnp.int32, (rows, depth), 0)
    hit = row == piv_ref[...]
    return hit, jnp.max(jnp.where(hit, 1.0, 0.0), axis=1, keepdims=True) > 0.0


def solve_kernel(first_row, panel_ref, upper_ref, piv_ref, out_ref):
    hit, is_pivot = hits(first_row[0], out_ref.shape[0], piv_ref)
    solved = dot3(split(panel_ref[...]), split(upper_ref[...]))
    out_ref[...] = jnp.where(is_pivot, jnp.where(hit, -1.0, 0.0), solved)


def solve(panel, inv_upper, pivots, first_row, part, rows):
    depth = panel.shape[1]
    return pl.pallas_call(
        solve_kernel,
        grid_spec=pltpu.PrefetchScalarGridSpec(
            num_scalar_prefetch=1,
            grid=(1,),
            in_specs=[
                pl.BlockSpec((rows, depth), lambda i, s: (part, 0)),
                pl.BlockSpec((depth, depth), lambda i, s: (0, 0)),
                pl.BlockSpec((1, depth), lambda i, s: (0, 0)),
            ],
            out_specs=pl.BlockSpec((rows, depth), lambda i, s: (0, 0)),
        ),
        out_shape=jax.ShapeDtypeStruct((rows, depth), jnp.float32),
        cost_estimate=cost(6 * rows * depth * depth, 4 * depth * (2 * rows + depth)),
        name="solve",
    )(first_row + part * rows, panel, inv_upper, pivots)


def clear_kernel(piv_ref, slab_ref, out_ref):
    _, is_pivot = hits(pl.program_id(0) * out_ref.shape[0], out_ref.shape[0], piv_ref)
    out_ref[...] = jnp.where(is_pivot, 0.0, slab_ref[...])


def clear(slab, pivots):
    rows, cols = slab.shape
    block = next(b for b in (512, 256, 128, 64, 32, 16, 8) if rows % b == 0)
    moved = pl.BlockSpec((block, cols), lambda i: (i, 0))
    return pl.pallas_call(
        clear_kernel,
        grid=(rows // block,),
        in_specs=[pl.BlockSpec(pivots.shape, lambda i: (0, 0)), moved],
        out_specs=moved,
        out_shape=jax.ShapeDtypeStruct(slab.shape, jnp.float32),
        cost_estimate=cost(rows * cols * 64, 8 * rows * cols),
        name="clear",
    )(pivots, slab)


def prepare_kernel(lower_ref, first_ref, second_ref, uh_ref, ul_ref):
    rows = split(first_ref[...] + second_ref[...])
    uh_ref[...], ul_ref[...] = split(dot3(split(lower_ref[...]), rows))


def prepare(inv_lower, first, second):
    depth, cols = first.shape
    half = jax.ShapeDtypeStruct((depth, cols), jnp.bfloat16)
    return pl.pallas_call(
        prepare_kernel,
        out_shape=[half, half],
        cost_estimate=cost(6 * depth * depth * cols, 4 * depth * (depth + 3 * cols)),
        name="prepare",
    )(inv_lower, first, second)


def update_kernel(count, table, *refs):
    pieces, (uh_ref, ul_ref, old_ref, out_ref) = refs[:count], refs[count:]
    upper = uh_ref[...], ul_ref[...]
    for k, piece in enumerate(pieces):
        rows = pl.ds(k * piece.shape[0], piece.shape[0])
        out_ref[rows, :] = old_ref[rows, :] - dot3(split(piece[...]), upper)


def update(entry, table, pieces, upper, held):
    rows, depth = pieces[0].shape
    cols = held.shape[1]
    total = rows * len(pieces)
    whole = lambda shape: pl.BlockSpec(shape, lambda i, table: (0, 0))
    moved = pl.BlockSpec((total, cols), lambda i, table: (table[entry], 0))
    return pl.pallas_call(
        functools.partial(update_kernel, len(pieces)),
        grid_spec=pltpu.PrefetchScalarGridSpec(
            num_scalar_prefetch=1,
            grid=(1,),
            in_specs=[whole((rows, depth))] * len(pieces) + [whole((depth, cols))] * 2 + [moved],
            out_specs=moved,
        ),
        out_shape=jax.ShapeDtypeStruct(held.shape, jnp.float32),
        input_output_aliases={len(pieces) + 3: 0},
        cost_estimate=cost(6 * total * depth * cols, 4 * (total * (depth + 2 * cols) + depth * cols)),
        name="update",
    )(table, *pieces, *upper, held)


def line_plan(top, bottom, me):
    z, y = me // 2, me % 2
    send = lambda value, pairs: lax.ppermute(value, "pcol", [(a * 2 + u, b * 2 + v) for a, b in pairs for u, v in ((0, 0), (1, 1))])
    cross = lambda value: lax.ppermute(value, "pcol", [(i, i ^ 1) for i in range(8)])
    ends, middle, outward = ((0, 1), (1, 0), (2, 3), (3, 2)), ((1, 2), (2, 1)), ((1, 0), (2, 3))
    inner = (z == 1) | (z == 2)
    own = top, bottom
    first, relay, side = [], [], []
    for half in own:
        first.append(send(half, ends))
        relay.append(send(half, middle))
        side.append(cross(half))
    side_first = [cross(first[0]), None]
    second, third_relay = [], []
    for k in range(2):
        second.append(jnp.where(inner, relay[k], send(relay[k], outward)))
        third_relay.append(send(first[k], middle))
    third = [jnp.where(inner, third_relay[k], send(third_relay[k], outward)) for k in range(2)]
    side_first[1] = send(side[1], ends)
    side_second = [cross(half) for half in second]
    side_third = [cross(half) for half in third]
    z1, z2, z3 = z ^ 1, jnp.where(z < 2, 2, 1), jnp.where(z < 2, 3, 0)
    return [
        (z * 2 + y, None, own),
        (z1 * 2 + y, None, first),
        (z * 2 + 1 - y, None, side),
        (z2 * 2 + y, None, second),
        (z2 * 2 + 1 - y, None, side_second),
        (z3 * 2 + y, None, third),
        (z1 * 2 + 1 - y, None, side_first),
        (z3 * 2 + 1 - y, 0, side_third[:1]),
        (z3 * 2 + 1 - y, 1, side_third[1:]),
    ]


def gather_plan(halves, n_pcol):
    me = lax.axis_index("pcol")
    if n_pcol == 8:
        return line_plan(*halves, me)
    rows = 2 * halves[0].shape[0]
    whole = lax.all_gather(jnp.concatenate(halves), "pcol", axis=0, tiled=True)
    return [(jnp.int32(j), None, [whole[j * rows : (j + 1) * rows]]) for j in range(n_pcol)]


def sum_over_prow(value, n_prow):
    if n_prow & (n_prow - 1) or n_prow < 2:
        total = lax.psum(value, "prow")
        return total, jnp.zeros_like(total)
    step = 1
    while True:
        other = lax.ppermute(value, "prow", [(i, i ^ step) for i in range(n_prow)])
        step *= 2
        if step == n_prow:
            return value, other
        value = value + other


def local(n_prow, n_pcol, slab, panel, pivots, inv_lower, inv_upper):
    row_count = slab.shape[0]
    rows = panel.shape[0]
    half = rows // 2
    local_index = pivots - lax.axis_index("prow") * row_count
    local_row = local_index[None, :]
    first_row = (lax.axis_index("pcol") * rows).astype(jnp.int32)[None]
    halves = [solve(panel, inv_upper, local_row, first_row, part, half) for part in range(2)]
    plan = gather_plan(halves, n_pcol)

    inside = (local_index >= 0) & (local_index < row_count)
    safe_index = jnp.where(inside, local_index, 0)
    picked = jnp.where(inside[:, None], jnp.take(slab, safe_index, axis=0), 0.0)
    upper = prepare(inv_lower, *sum_over_prow(picked, n_prow))

    table = jnp.stack([owner if part is None else owner * 2 + part for owner, part, _ in plan]).astype(jnp.int32)
    updated = clear(slab, local_row)
    for entry, (_, _, pieces) in enumerate(plan):
        updated = update(entry, table, pieces, upper, updated)
    return updated


def solution(mesh):
    return jax.shard_map(
        functools.partial(local, mesh.shape["prow"], mesh.shape["pcol"]),
        mesh=mesh,
        in_specs=(P("prow", "pcol"), P(("prow", "pcol"), None), P(), P(), P()),
        out_specs=P("prow", "pcol"),
        check_vma=False,
    )
```

```python
import functools

import jax
import jax.numpy as jnp
import numpy as np
from jax import lax
from jax.experimental import pallas as pl
from jax.experimental.pallas import tpu as pltpu
from jax.sharding import PartitionSpec as P


def split(value):
    high = value.astype(jnp.bfloat16)
    low = (value - high.astype(jnp.float32)).astype(jnp.bfloat16)
    return high, low


def dot3(left, right):
    dot = functools.partial(jnp.dot, preferred_element_type=jnp.float32)
    return dot(left[0], right[0]) + (dot(left[0], right[1]) + dot(left[1], right[0]))


def cost(flops, moved):
    return pl.CostEstimate(flops=flops, bytes_accessed=moved, transcendentals=0)


def hits(first_row, rows, piv_ref):
    depth = piv_ref.shape[1]
    row = first_row + lax.broadcasted_iota(jnp.int32, (rows, depth), 0)
    hit = row == piv_ref[...]
    return hit, jnp.max(jnp.where(hit, 1.0, 0.0), axis=1, keepdims=True) > 0.0


def solve_kernel(first_row, panel_ref, upper_ref, piv_ref, *refs):
    out_ref, token_ref = refs[-2:]
    token_ref[...] = jnp.zeros_like(token_ref)
    hit, is_pivot = hits(first_row[0], out_ref.shape[0], piv_ref)
    solved = dot3(split(panel_ref[...]), split(upper_ref[...]))
    out_ref[...] = jnp.where(is_pivot, jnp.where(hit, -1.0, 0.0), solved)


def solve(panel, inv_upper, pivots, first_row, part, rows, *earlier):
    depth = panel.shape[1]
    return pl.pallas_call(
        solve_kernel,
        grid_spec=pltpu.PrefetchScalarGridSpec(
            num_scalar_prefetch=1,
            grid=(1,),
            in_specs=[
                pl.BlockSpec((rows, depth), lambda i, s: (part, 0)),
                pl.BlockSpec((depth, depth), lambda i, s: (0, 0)),
                pl.BlockSpec((1, depth), lambda i, s: (0, 0)),
            ]
            + [pl.BlockSpec(memory_space=pl.ANY)] * len(earlier),
            out_specs=[pl.BlockSpec((rows, depth), lambda i, s: (0, 0)), pl.BlockSpec((8, 128), lambda i, s: (0, 0))],
        ),
        out_shape=[
            jax.ShapeDtypeStruct((rows, depth), jnp.float32),
            jax.ShapeDtypeStruct((8, 128), jnp.int32),
        ],
        cost_estimate=cost(6 * rows * depth * depth, 4 * depth * (2 * rows + depth)),
        name="solve",
    )(first_row + part * rows, panel, inv_upper, pivots, *earlier)


def after(value, token):
    return value + token[0, 0].astype(value.dtype)


def clear_kernel(piv_ref, slab_ref, out_ref, token_ref):
    token_ref[...] = jnp.zeros_like(token_ref)
    _, is_pivot = hits(pl.program_id(0) * out_ref.shape[0], out_ref.shape[0], piv_ref)
    out_ref[...] = jnp.where(is_pivot, 0.0, slab_ref[...])


def clear(slab, pivots):
    rows, cols = slab.shape
    block = next(b for b in (512, 256, 128, 64, 32, 16, 8) if rows % b == 0)
    moved = pl.BlockSpec((block, cols), lambda i: (i, 0))
    return pl.pallas_call(
        clear_kernel,
        grid=(rows // block,),
        in_specs=[pl.BlockSpec(pivots.shape, lambda i: (0, 0)), moved],
        out_specs=[moved, pl.BlockSpec((8, 128), lambda i: (0, 0))],
        out_shape=[
            jax.ShapeDtypeStruct(slab.shape, jnp.float32),
            jax.ShapeDtypeStruct((8, 128), jnp.float32),
        ],
        cost_estimate=cost(rows * cols * 64, 8 * rows * cols),
        name="clear",
    )(pivots, slab)


def prepare_kernel(lower_ref, first_ref, second_ref, uh_ref, ul_ref):
    rows = split(first_ref[...] + second_ref[...])
    uh_ref[...], ul_ref[...] = split(dot3(split(lower_ref[...]), rows))


def prepare(inv_lower, first, second):
    depth, cols = first.shape
    half = jax.ShapeDtypeStruct((depth, cols), jnp.bfloat16)
    return pl.pallas_call(
        prepare_kernel,
        out_shape=[half, half],
        cost_estimate=cost(6 * depth * depth * cols, 4 * depth * (depth + 3 * cols)),
        name="prepare",
    )(inv_lower, first, second)


def update_kernel(count, table, *refs):
    pieces, (uh_ref, ul_ref, old_ref, out_ref, token_ref) = refs[:count], refs[count:]
    token_ref[...] = jnp.zeros_like(token_ref)
    upper = uh_ref[...], ul_ref[...]
    for k, piece in enumerate(pieces):
        rows = pl.ds(k * piece.shape[0], piece.shape[0])
        out_ref[rows, :] = old_ref[rows, :] - dot3(split(piece[...]), upper)


def update(entry, table, pieces, upper, held):
    rows, depth = pieces[0].shape
    cols = held.shape[1]
    total = rows * len(pieces)
    whole = lambda shape: pl.BlockSpec(shape, lambda i, table: (0, 0))
    moved = pl.BlockSpec((total, cols), lambda i, table: (table[entry], 0))
    return pl.pallas_call(
        functools.partial(update_kernel, len(pieces)),
        grid_spec=pltpu.PrefetchScalarGridSpec(
            num_scalar_prefetch=1,
            grid=(1,),
            in_specs=[whole((rows, depth))] * len(pieces) + [whole((depth, cols))] * 2 + [moved],
            out_specs=[moved, whole((8, 128))],
        ),
        out_shape=[
            jax.ShapeDtypeStruct(held.shape, jnp.float32),
            jax.ShapeDtypeStruct((8, 128), jnp.float32),
        ],
        input_output_aliases={len(pieces) + 3: 0},
        cost_estimate=cost(6 * total * depth * cols, 4 * (total * (depth + 2 * cols) + depth * cols)),
        name="update",
    )(table, *pieces, *upper, held)


def line_product(solved, pick, finish, clear_slab):
    me = lax.axis_index("pcol")
    z, y = me // 2, me % 2
    send = lambda value, pairs: lax.ppermute(value, "pcol", [(a * 2 + u, b * 2 + u) for a, b in pairs for u in range(2)])
    cross = lambda value: lax.ppermute(value, "pcol", [(i, i ^ 1) for i in range(8)])
    ends, middle, outward = ((0, 1), (1, 0), (2, 3), (3, 2)), ((1, 2), (2, 1)), ((1, 0), (2, 3))
    inner = (z == 1) | (z == 2)
    z1, z2, z3 = z ^ 1, jnp.where(z < 2, 2, 1), jnp.where(z < 2, 3, 0)
    owners = [z * 2 + y, z1 * 2 + y, z * 2 + 1 - y, z2 * 2 + y, z2 * 2 + 1 - y, z3 * 2 + y, z1 * 2 + 1 - y]
    last = z3 * 2 + 1 - y
    table = jnp.stack(owners + [last * 2, last * 2 + 1]).astype(jnp.int32)

    first, relay, side = [], [], []
    own = []
    for k in range(2):
        if k == 0:
            piece, token = solved(k)
            picked = pick(token)
        else:
            piece, _ = solved(k, picked)
        own.append(piece)
        first.append(send(piece, ends))
        relay.append(send(piece, middle))
        side.append(cross(piece))
    upper = finish(picked)
    held, token = clear_slab()
    side_first = [cross(first[0]), None]
    outer_second = [send(relay[k], outward) for k in range(2)]
    third_relay = [send(first[k], middle) for k in range(2)]
    second = [jnp.where(inner, relay[k], outer_second[k]) for k in range(2)]
    second[0] = after(second[0], token)
    side_second = [cross(piece) for piece in second]
    outer_third = [send(third_relay[k], outward) for k in range(2)]
    third = [jnp.where(inner, third_relay[k], outer_third[k]) for k in range(2)]
    side_first[1] = send(lax.optimization_barrier((side[1], outer_third[0]))[0], ends)
    held, _ = update(0, table, own, upper, held)
    held, token = update(1, table, first, upper, held)
    third[0] = after(third[0], token)
    side_third = [cross(third[0])]
    held, _ = update(2, table, side, upper, held)
    held, token = update(3, table, second, upper, held)
    third[1] = after(third[1], token)
    side_third.append(cross(third[1]))
    held, _ = update(4, table, side_second, upper, held)
    held, _ = update(5, table, third, upper, held)
    held, _ = update(6, table, side_first, upper, held)
    held, _ = update(7, table, side_third[:1], upper, held)
    return update(8, table, side_third[1:], upper, held)[0]


def gathered_product(halves, upper, held, n_pcol):
    rows = 2 * halves[0].shape[0]
    whole = lax.all_gather(jnp.concatenate(halves), "pcol", axis=0, tiled=True)
    table = jnp.arange(n_pcol, dtype=jnp.int32)
    for j in range(n_pcol):
        held, _ = update(j, table, [whole[j * rows : (j + 1) * rows]], upper, held)
    return held


def sum_over_prow(value, n_prow):
    if n_prow & (n_prow - 1) or n_prow < 2:
        total = lax.psum(value, "prow")
        return total, jnp.zeros_like(total)
    step = 1
    while True:
        other = lax.ppermute(value, "prow", [(i, i ^ step) for i in range(n_prow)])
        step *= 2
        if step == n_prow:
            return value, other
        value = value + other


def local(n_prow, n_pcol, slab, panel, pivots, inv_lower, inv_upper):
    row_count = slab.shape[0]
    rows = panel.shape[0]
    half = rows // 2
    local_index = pivots - lax.axis_index("prow") * row_count
    local_row = local_index[None, :]
    first_row = (lax.axis_index("pcol") * rows).astype(jnp.int32)[None]
    inside = (local_index >= 0) & (local_index < row_count)
    safe_index = jnp.where(inside, local_index, 0)
    solved = lambda k, *earlier: solve(panel, inv_upper, local_row, first_row, k, half, *earlier)
    pick = lambda token: jnp.where(inside[:, None], jnp.take(slab, after(safe_index, token), axis=0), 0.0)
    finish = lambda picked: prepare(inv_lower, *sum_over_prow(picked, n_prow))
    if n_pcol == 8:
        return line_product(solved, pick, finish, lambda: clear(slab, local_row))
    halves, tokens = zip(*[solved(part) for part in range(2)])
    return gathered_product(halves, finish(pick(tokens[0])), clear(slab, local_row)[0], n_pcol)


def solution(mesh):
    return jax.shard_map(
        functools.partial(local, mesh.shape["prow"], mesh.shape["pcol"]),
        mesh=mesh,
        in_specs=(P("prow", "pcol"), P(("prow", "pcol"), None), P(), P(), P()),
        out_specs=P("prow", "pcol"),
        check_vma=False,
    )
```

```python
import functools

import jax
import jax.numpy as jnp
import numpy as np
from jax import lax
from jax.experimental import pallas as pl
from jax.experimental.pallas import tpu as pltpu
from jax.sharding import PartitionSpec as P


def split(value):
    high = value.astype(jnp.bfloat16)
    low = (value - high.astype(jnp.float32)).astype(jnp.bfloat16)
    return high, low


def dot3(left, right):
    dot = functools.partial(jnp.dot, preferred_element_type=jnp.float32)
    return dot(left[0], right[0]) + (dot(left[0], right[1]) + dot(left[1], right[0]))


def cost(flops, moved):
    return pl.CostEstimate(flops=flops, bytes_accessed=moved, transcendentals=0)


def hits(first_row, rows, piv_ref):
    depth = piv_ref.shape[1]
    row = first_row + lax.broadcasted_iota(jnp.int32, (rows, depth), 0)
    hit = row == piv_ref[...]
    return hit, jnp.max(jnp.where(hit, 1.0, 0.0), axis=1, keepdims=True) > 0.0


def solve_kernel(first_row, panel_ref, upper_ref, piv_ref, *refs):
    out_ref, token_ref = refs[-2:]
    token_ref[...] = jnp.zeros_like(token_ref)
    hit, is_pivot = hits(first_row[0], out_ref.shape[0], piv_ref)
    solved = dot3(split(panel_ref[...]), split(upper_ref[...]))
    out_ref[...] = jnp.where(is_pivot, jnp.where(hit, -1.0, 0.0), solved)


def solve(panel, inv_upper, pivots, first_row, part, rows, *earlier):
    depth = panel.shape[1]
    return pl.pallas_call(
        solve_kernel,
        grid_spec=pltpu.PrefetchScalarGridSpec(
            num_scalar_prefetch=1,
            grid=(1,),
            in_specs=[
                pl.BlockSpec((rows, depth), lambda i, s: (part, 0)),
                pl.BlockSpec((depth, depth), lambda i, s: (0, 0)),
                pl.BlockSpec((1, depth), lambda i, s: (0, 0)),
            ]
            + [pl.BlockSpec(memory_space=pl.ANY)] * len(earlier),
            out_specs=[pl.BlockSpec((rows, depth), lambda i, s: (0, 0)), pl.BlockSpec((1, depth), lambda i, s: (0, 0))],
        ),
        out_shape=[
            jax.ShapeDtypeStruct((rows, depth), jnp.float32),
            jax.ShapeDtypeStruct((1, depth), jnp.int32),
        ],
        cost_estimate=cost(6 * rows * depth * depth, 4 * depth * (2 * rows + depth)),
        name="solve",
    )(first_row + part * rows, panel, inv_upper, pivots, *earlier)


def after(value, token):
    return value + token.reshape((1,) * (value.ndim - 1) + (-1,))


def clear_kernel(piv_ref, slab_ref, *refs):
    out_ref, token_ref = refs[-2:]
    token_ref[...] = jnp.zeros_like(token_ref)
    _, is_pivot = hits(pl.program_id(0) * out_ref.shape[0], out_ref.shape[0], piv_ref)
    out_ref[...] = jnp.where(is_pivot, 0.0, slab_ref[...])


def clear(slab, pivots, *earlier):
    rows, cols = slab.shape
    depth = pivots.shape[1]
    block = next(b for b in (512, 256, 128, 64, 32, 16, 8) if rows % b == 0)
    moved = pl.BlockSpec((block, cols), lambda i: (i, 0))
    return pl.pallas_call(
        clear_kernel,
        grid=(rows // block,),
        in_specs=[pl.BlockSpec(pivots.shape, lambda i: (0, 0)), moved]
        + [pl.BlockSpec(memory_space=pl.ANY)] * len(earlier),
        out_specs=[moved, pl.BlockSpec((1, depth), lambda i: (0, 0))],
        out_shape=[
            jax.ShapeDtypeStruct(slab.shape, jnp.float32),
            jax.ShapeDtypeStruct((1, depth), jnp.float32),
        ],
        cost_estimate=cost(rows * cols * 64, 8 * rows * cols),
        name="clear",
    )(pivots, slab, *earlier)


def prepare_kernel(lower_ref, first_ref, second_ref, uh_ref, ul_ref):
    rows = split(first_ref[...] + second_ref[...])
    uh_ref[...], ul_ref[...] = split(dot3(split(lower_ref[...]), rows))


def prepare(inv_lower, first, second):
    depth, cols = first.shape
    half = jax.ShapeDtypeStruct((depth, cols), jnp.bfloat16)
    return pl.pallas_call(
        prepare_kernel,
        out_shape=[half, half],
        cost_estimate=cost(6 * depth * depth * cols, 4 * depth * (depth + 3 * cols)),
        name="prepare",
    )(inv_lower, first, second)


def update_kernel(count, table, *refs):
    pieces, (uh_ref, ul_ref, old_ref), (out_ref, token_ref) = refs[:count], refs[count : count + 3], refs[-2:]
    token_ref[...] = jnp.zeros_like(token_ref)
    upper = uh_ref[...], ul_ref[...]
    for k, piece in enumerate(pieces):
        rows = pl.ds(k * piece.shape[0], piece.shape[0])
        out_ref[rows, :] = old_ref[rows, :] - dot3(split(piece[...]), upper)


def update(entry, table, pieces, upper, held, *earlier):
    rows, depth = pieces[0].shape
    cols = held.shape[1]
    total = rows * len(pieces)
    whole = lambda shape: pl.BlockSpec(shape, lambda i, table: (0, 0))
    moved = pl.BlockSpec((total, cols), lambda i, table: (table[entry], 0))
    return pl.pallas_call(
        functools.partial(update_kernel, len(pieces)),
        grid_spec=pltpu.PrefetchScalarGridSpec(
            num_scalar_prefetch=1,
            grid=(1,),
            in_specs=[whole((rows, depth))] * len(pieces) + [whole((depth, cols))] * 2 + [moved]
            + [pl.BlockSpec(memory_space=pl.ANY)] * len(earlier),
            out_specs=[moved, whole((1, depth))],
        ),
        out_shape=[
            jax.ShapeDtypeStruct(held.shape, jnp.float32),
            jax.ShapeDtypeStruct((1, depth), jnp.float32),
        ],
        input_output_aliases={len(pieces) + 3: 0},
        cost_estimate=cost(6 * total * depth * cols, 4 * (total * (depth + 2 * cols) + depth * cols)),
        name="update",
    )(table, *pieces, *upper, held, *earlier)


def line_product(solved, pick, add_up, finish, clear_slab):
    me = lax.axis_index("pcol")
    z, y = me // 2, me % 2
    send = lambda value, pairs: lax.ppermute(value, "pcol", [(a * 2 + u, b * 2 + u) for a, b in pairs for u in range(2)])
    cross = lambda value: lax.ppermute(value, "pcol", [(i, i ^ 1) for i in range(8)])
    ends, middle, outward = ((0, 1), (1, 0), (2, 3), (3, 2)), ((1, 2), (2, 1)), ((1, 0), (2, 3))
    inner = (z == 1) | (z == 2)
    z1, z2, z3 = z ^ 1, jnp.where(z < 2, 2, 1), jnp.where(z < 2, 3, 0)
    owners = [z * 2 + y, z1 * 2 + y, z * 2 + 1 - y, z2 * 2 + y, z2 * 2 + 1 - y, z3 * 2 + y, z1 * 2 + 1 - y]
    last = z3 * 2 + 1 - y
    table = jnp.stack(owners + [last * 2, last * 2 + 1]).astype(jnp.int32)

    first, relay, side = [], [], []
    own = []
    for k in range(2):
        piece, token = solved(k)
        own.append(piece)
        first.append(send(piece, ends))
        relay.append(send(piece, middle))
        side.append(cross(piece))
    addends = add_up(pick(token))
    upper = finish(*addends)
    held, token = clear_slab(addends[0])
    side_first = [cross(first[0]), None]
    outer_second = [send(relay[k], outward) for k in range(2)]
    third_relay = [send(first[k], middle) for k in range(2)]
    second = [jnp.where(inner, relay[k], outer_second[k]) for k in range(2)]
    second[0] = after(second[0], token)
    side_second = [cross(piece) for piece in second]
    outer_third = [send(third_relay[k], outward) for k in range(2)]
    third = [jnp.where(inner, third_relay[k], outer_third[k]) for k in range(2)]
    side_first[1] = send(lax.optimization_barrier((side[1], outer_third[0]))[0], ends)
    held, _ = update(0, table, own, upper, held)
    held, token = update(1, table, first, upper, held)
    third[0] = after(third[0], token)
    side_third = [cross(third[0])]
    held, _ = update(2, table, side, upper, held)
    held, token = update(3, table, second, upper, held, third[0])
    third[1] = after(third[1], token)
    side_third.append(cross(third[1]))
    held, _ = update(4, table, side_second, upper, held)
    held, _ = update(5, table, third, upper, held)
    held, _ = update(6, table, side_first, upper, held)
    held, _ = update(7, table, side_third[:1], upper, held)
    return update(8, table, side_third[1:], upper, held)[0]


def gathered_product(halves, upper, held, n_pcol):
    rows = 2 * halves[0].shape[0]
    whole = lax.all_gather(jnp.concatenate(halves), "pcol", axis=0, tiled=True)
    table = jnp.arange(n_pcol, dtype=jnp.int32)
    for j in range(n_pcol):
        held, _ = update(j, table, [whole[j * rows : (j + 1) * rows]], upper, held)
    return held


def sum_over_prow(value, n_prow):
    if n_prow & (n_prow - 1) or n_prow < 2:
        total = lax.psum(value, "prow")
        return total, jnp.zeros_like(total)
    step = 1
    while True:
        other = lax.ppermute(value, "prow", [(i, i ^ step) for i in range(n_prow)])
        step *= 2
        if step == n_prow:
            return value, other
        value = value + other


def local(n_prow, n_pcol, slab, panel, pivots, inv_lower, inv_upper):
    row_count = slab.shape[0]
    rows = panel.shape[0]
    half = rows // 2
    local_index = pivots - lax.axis_index("prow") * row_count
    local_row = local_index[None, :]
    first_row = (lax.axis_index("pcol") * rows).astype(jnp.int32)[None]
    inside = (local_index >= 0) & (local_index < row_count)
    safe_index = jnp.where(inside, local_index, 0)
    solved = lambda k, *earlier: solve(panel, inv_upper, local_row, first_row, k, half, *earlier)
    pick = lambda token: jnp.where(inside[:, None], jnp.take(slab, after(safe_index, token), axis=0), 0.0)
    add_up = lambda picked: sum_over_prow(picked, n_prow)
    finish = lambda *addends: prepare(inv_lower, *addends)
    if n_pcol == 8:
        return line_product(solved, pick, add_up, finish, lambda earlier: clear(slab, local_row, earlier))
    halves, tokens = zip(*[solved(part) for part in range(2)])
    return gathered_product(halves, finish(*add_up(pick(tokens[0]))), clear(slab, local_row)[0], n_pcol)


def solution(mesh):
    return jax.shard_map(
        functools.partial(local, mesh.shape["prow"], mesh.shape["pcol"]),
        mesh=mesh,
        in_specs=(P("prow", "pcol"), P(("prow", "pcol"), None), P(), P(), P()),
        out_specs=P("prow", "pcol"),
        check_vma=False,
    )
```
